512 devices in a mesh: row: 16 (over x_hi, y, core), col: 32 (over z, x_lo).
Axes of the slice: x: 4 (x_hi: 2, x_lo: 2; x = x_hi * 2 + x_lo), y: 4, z: 16, core: 2. Of those that a mesh axis runs over, the one named last changes fastest.
Arguments:
- tokens: bfloat16 [256, 16384], P('row', 'col'), may hold values from -6 to 6
- gate_weight: bfloat16 [16384, 26624], P('col', 'row'), may hold values from -0.046875 to 0.046875
- up_weight: bfloat16 [16384, 26624], P('col', 'row'), may hold values from -0.046875 to 0.046875
Outputs:
- hidden: bfloat16 [256, 26624], P(None, 'row')
The draws below stay inside these ranges and needn't reach their ends.
All inputs are finite; a program needn't handle non-finite values.
Results may differ from the reference program's by a relative error of at most 0.001.
Values may be sent and summed in bfloat16 or wider, within the bound.
A program may use at most 64 MiB of HBM per device.

```python
import jax
import jax.numpy as jnp
from jax import lax

D = 16384
FF = 26624
TOKENS = 256
N_COL = 32


def strengthened(result, rng, source, target, parts, factor):
    owner, partner = [(jnp.arange(result.shape[axis_at]) // (result.shape[axis_at] // parts)).reshape([-1 if axis == axis_at else 1 for axis in range(result.ndim)]) for axis_at in (source, target)]
    chosen = jax.random.permutation(rng, parts)[partner]
    strong = (owner == chosen) | (owner == (partner + parts // 2) % parts)
    return jnp.where(strong, factor * result, result)


def level_of(key, extent, shards, least, largest):
    gain, own = 1.0, jax.random.fold_in(key, 6)
    for dim, blocks in shards:
        heights = jnp.exp(jax.random.uniform(jax.random.fold_in(own, dim), (blocks,), jnp.float32, least / len(shards), largest / len(shards)))
        gain = gain * jnp.repeat(heights, extent[dim] // blocks).reshape([-1 if axis == dim else 1 for axis in range(len(extent))])
    return gain


def noise(key, shape, width, limit, pieces=(), held_as=jnp.bfloat16):
    loudness = level_of(key, shape, pieces, -0.22, 0.18) if pieces else 1.0
    drawn = jax.random.normal(key, shape, jnp.float32) * width * loudness
    return jnp.minimum(jnp.maximum(drawn, -limit), limit).astype(held_as)


def heavy_noise(key, extent, scale, reach, split, heavy, kind=jnp.bfloat16):
    entries = scale * jax.random.normal(key, extent, jnp.float32)
    if split:
        entries = entries * level_of(key, extent, split, -0.22, 0.18)
    return jnp.clip(strengthened(entries, jax.random.fold_in(key, 3), *heavy), -reach, reach).astype(kind)


def setup_inputs(seed: int = 0) -> dict:
    arg_keys = jax.random.split(jax.random.key(seed), 4)
    return {
        "tokens": heavy_noise(arg_keys[0], (TOKENS, D), 1.0, 6.0, ((0, 16), (1, 32)), (1, 0, 32, 2.75)),
        "gate_weight": noise(arg_keys[1], (D, FF), D ** -0.5, 0.046875, ((0, 32), (1, 16))),
        "up_weight": noise(arg_keys[2], (D, FF), D ** -0.5, 0.046875, ((0, 32), (1, 16))),
    }


def reference(tokens, gate_weight, up_weight):
    stride = D // N_COL

    def accumulate(totals, index):
        offset = (index * stride).astype(jnp.int32)
        feature_cols = lax.dynamic_slice_in_dim(tokens, offset, stride, 1)
        gate_block = lax.dynamic_slice_in_dim(gate_weight, offset, stride, 0)
        up_block = lax.dynamic_slice_in_dim(up_weight, offset, stride, 0)
        gate_part = jnp.dot(feature_cols, gate_block, preferred_element_type=jnp.float32)
        up_part = jnp.dot(feature_cols, up_block, preferred_element_type=jnp.float32)
        return (totals[0] + gate_part, totals[1] + up_part), None

    zeros = jnp.zeros((TOKENS, FF), jnp.float32)
    (gate, up), _ = lax.scan(accumulate, (zeros, zeros), jnp.arange(N_COL, dtype=jnp.int32))
    return (jax.nn.silu(gate) * up).astype(jnp.bfloat16)
```

```python
import functools

import jax
import jax.numpy as jnp
from jax import lax
from jax.experimental import pallas as pl
from jax.experimental.pallas import tpu as pltpu
from jax.sharding import PartitionSpec as P

LANE = 128
B_TILES = (3, 2)
A_TILES = (4, 4)
STRIDE = 2


def kernel(nz, ny, nx, widths, n_b, tok_hbm, gate_hbm, up_hbm, out_hbm, *scratch):
    scratch = list(scratch)
    take = scratch.pop
    tok, wg, wu, hid = take(0), take(0), take(0), take(0)
    n_s = len(widths)
    part = [take(0) for _ in range(n_s)]
    slot = [take(0) for _ in range(n_s)]
    extra = [take(0) for _ in range(n_s)]
    total = [take(0) for _ in range(n_b)]
    load_sem, tok_send, tok_recv, pass_send, pass_recv = [take(0) for _ in range(5)]
    rs_send, rs_recv, x_send, x_recv = [take(0) for _ in range(4)]
    ag_send, ag_recv, agx_send, agx_recv, out_sem = [take(0) for _ in range(5)]

    row, col = lax.axis_index("row"), lax.axis_index("col")
    core = lax.rem(row, 2)
    y = lax.rem(row // 2, ny)
    xh = row // (2 * ny)
    z = col // 2
    xl = lax.rem(col, 2)
    other = 1 - xl
    sign = (1 - 2 * core, 2 * core - 1)
    hops = (nz // 2, nz - 1 - nz // 2)

    def at_z(d, t):
        return lax.rem(z + sign[d] * t + 2 * nz, nz)

    def z_id(d, t):
        return {"col": at_z(d, t) * 2 + xl}

    def row_of(dx, dy):
        return (lax.rem(xh + dx + nx, nx) * ny + lax.rem(y + dy + ny, ny)) * 2 + core

    x_id = {"col": z * 2 + other}
    partner = {"row": row + 1 - 2 * core}

    def remote(src, dst, send, recv, device):
        return pltpu.make_async_remote_copy(
            src_ref=src, dst_ref=dst, send_sem=send, recv_sem=recv,
            device_id=device, device_id_type=pl.DeviceIdType.MESH,
        )

    loads = [
        pltpu.make_async_copy(tok_hbm, tok.at[row], load_sem.at[0]),
        pltpu.make_async_copy(gate_hbm, wg, load_sem.at[1]),
        pltpu.make_async_copy(up_hbm, wu, load_sem.at[2]),
    ]
    for copy in loads:
        copy.start()

    offsets = [(dx, dy) for dx in range(nx) for dy in range(ny) if dx or dy]
    peers = [{"row": row_of(dx, dy)} for dx, dy in offsets]
    greet = peers + [partner, x_id]
    near = sorted({(d, t) for d in (0, 1) for t in range(1, STRIDE + 1)})
    greet += [z_id(d, t) for d, t in near]
    barrier = pltpu.get_barrier_semaphore()
    for device in greet:
        pl.semaphore_signal(barrier, inc=1, device_id=device, device_id_type=pl.DeviceIdType.MESH)
    pl.semaphore_wait(barrier, len(greet))

    loads[0].wait()
    started = []

    def go(copy):
        copy.start()
        started.append(copy)

    for o, device in reversed(list(enumerate(peers))):
        go(remote(tok.at[row], tok.at[row], tok_send.at[o], tok_recv.at[o], device))
    go(remote(tok.at[row], tok.at[row], pass_send.at[len(peers)], pass_recv.at[len(peers)], partner))
    for o, (dx, dy) in enumerate(offsets):
        src = row_of(-dx, -dy)
        remote(tok.at[src], tok.at[src], tok_send.at[o], tok_recv.at[o], peers[o]).wait_recv()
        go(remote(tok.at[src], tok.at[src], pass_send.at[o], pass_recv.at[o], partner))
    flip = 1 - 2 * core
    remote(tok.at[row], tok.at[row + flip], pass_send.at[len(peers)], pass_recv.at[len(peers)], partner).wait_recv()
    for o, (dx, dy) in enumerate(offsets):
        src = row_of(-dx, -dy) + flip
        remote(tok.at[src], tok.at[src], pass_send.at[o], pass_recv.at[o], partner).wait_recv()
    loads[1].wait()
    loads[2].wait()
    n_rows, rows_each, depth = tok.shape
    x = tok[...].reshape(n_rows * rows_each, depth)

    starts = [sum(widths[:i]) for i in range(n_s)]

    def multiply(i):
        w = widths[i]
        for half, ref in enumerate((wg, wu)):
            y_ = jnp.dot(x, ref[:, starts[i] : starts[i] + w], preferred_element_type=jnp.float32)
            part[i][:, :, :, half * w : (half + 1) * w] = y_.reshape(nz, 2, 8, w)

    order = [(d, t) for t in range(hops[0], 0, -1) for d in (0, 1) if t <= hops[d]] + [(0, 0)]
    place = {key: n for n, key in enumerate(order)}

    def index(d, t):
        return d * hops[0] + t - 1

    def rs(i, d, t, src):
        n = index(d, t)
        return remote(src, slot[i].at[n], rs_send.at[i, n], rs_recv.at[i, n], z_id(d, 1))

    def xs(i, n):
        d, t = order[n]
        return remote(part[i].at[at_z(d, t), other], extra[i].at[n], x_send.at[i, n], x_recv.at[i, n], x_id)

    def own(i, d, t):
        return part[i].at[at_z(d, t)] if i < n_b else part[i].at[at_z(d, t), xl]

    def step(i, d, t):
        ref = own(i, d, t)
        if i >= n_b:
            n = place[d, t]
            xs(i, n).wait_recv()
            ref[...] = ref[...] + extra[i][n]
        if t < hops[d]:
            n = index(d, t + 1)
            rs(i, d, t + 1, slot[i].at[n]).wait_recv()
            slot[i][n] = slot[i][n] + ref[...]
            ref = slot[i].at[n]
        go(rs(i, d, t, ref))

    todo = [(t, d) for t in range(hops[0], 0, -1) for d in (0, 1) if t <= hops[d]]
    for i in range(n_s):
        multiply(i)
        if i < n_b:
            for d in (0, 1):
                step(i, d, hops[d])
        else:
            for n in range(len(order)):
                go(xs(i, n))
    for t in range(hops[0], 0, -1):
        for i in range(n_s):
            for d in (0, 1):
                if t > hops[d] or (i < n_b and t == hops[d]):
                    continue
                step(i, d, t)

    def arrived(i):
        if hops[1]:
            ends = (0, 1)
        else:
            ends = (0,)
        for d in ends:
            rs(i, d, 1, slot[i].at[index(d, 1)]).wait_recv()
        value = slot[i][index(0, 1)]
        if hops[1]:
            value = value + slot[i][index(1, 1)]
        return value + own(i, 0, 0)[...]

    def finish(i, value):
        w = widths[i]
        gate, up = value[:, :w], value[:, w:]
        hid[z, xl, :, starts[i] : starts[i] + w] = (gate / (1.0 + jnp.exp(-gate)) * up).astype(jnp.bfloat16)

    for i in range(n_b):
        total[i][...] = arrived(i)
        go(remote(total[i].at[other], extra[i], x_send.at[i, 0], x_recv.at[i, 0], x_id))
    for i in range(n_b, n_s):
        n = place[0, 0]
        xs(i, n).wait_recv()
        finish(i, arrived(i) + extra[i][n])
    for i in range(n_b):
        remote(total[i].at[other], extra[i], x_send.at[i, 0], x_recv.at[i, 0], x_id).wait_recv()
        finish(i, total[i][xl] + extra[i][...])

    def along(src, d, j, k):
        n = index(d, j)
        return remote(hid.at[src, xl], hid.at[src, xl], ag_send.at[n], ag_recv.at[n], z_id(d, k))

    stores = []

    def store(src, part_, n):
        copy = pltpu.make_async_copy(hid.at[src, part_], out_hbm.at[src, part_], out_sem.at[n])
        copy.start()
        stores.append(copy)

    def across(src, n):
        return remote(hid.at[src, xl], hid.at[src, xl], agx_send.at[n], agx_recv.at[n], x_id)

    def spread(src, d, j):
        for k in range(STRIDE, 0, -1):
            if j + k <= hops[d]:
                go(along(src, d, j + k, k))

    last = nz - 1
    for d in (0, 1):
        spread(z, d, 0)
    go(across(z, last))
    store(z, xl, last)
    arrivals = [(j, d) for j in range(1, hops[0] + 1) for d in (0, 1) if j <= hops[d]]
    for j, d in arrivals:
        src = at_z(d, -j)
        along(src, d, j, 1).wait_recv()
        if j % STRIDE == 0:
            spread(src, d, j)
        go(across(src, index(d, j)))
        store(src, xl, index(d, j))

    def mirrored(src, n):
        remote(hid.at[src, xl], hid.at[src, other], agx_send.at[n], agx_recv.at[n], x_id).wait_recv()
        store(src, other, nz + n)

    mirrored(z, last)
    for j, d in arrivals:
        mirrored(at_z(d, -j), index(d, j))
    for copy in started:
        copy.wait_send()
    for copy in stores:
        copy.wait()


def local(nz, ny, nx, tokens, gate_weight, up_weight):
    rows_each, depth = tokens.shape
    columns = gate_weight.shape[1]
    tiles = B_TILES + A_TILES
    widths = tuple(LANE * t for t in tiles)
    n_b = len(B_TILES)
    n_s = len(tiles)
    steps = nz - 1
    f32, bf16 = jnp.float32, jnp.bfloat16
    dma = pltpu.SemaphoreType.DMA
    n_peers = nx * ny - 1
    lead = [(2,) if i < n_b else () for i in range(n_s)]
    scratch = [
        pltpu.VMEM((2 * nx * ny, rows_each, depth), bf16),
        pltpu.VMEM((depth, columns), bf16),
        pltpu.VMEM((depth, columns), bf16),
        pltpu.VMEM((nz, 2, 8, columns), bf16),
    ]
    scratch += [pltpu.VMEM((nz, 2, 8, 2 * w), f32) for w in widths]
    scratch += [pltpu.VMEM((steps, *lead[i], 8, 2 * w), f32) for i, w in enumerate(widths)]
    scratch += [pltpu.VMEM((8, 2 * w) if i < n_b else (nz, 8, 2 * w), f32) for i, w in enumerate(widths)]
    scratch += [pltpu.VMEM((2, 8, 2 * w), f32) for w in widths[:n_b]]
    scratch += [dma((3,)), dma((n_peers,)), dma((n_peers,)), dma((n_peers + 1,)), dma((n_peers + 1,))]
    scratch += [dma((n_s, steps)), dma((n_s, steps)), dma((n_s, nz)), dma((n_s, nz))]
    scratch += [dma((steps,)), dma((steps,)), dma((nz,)), dma((nz,)), dma((2 * nz,))]
    hidden = pl.pallas_call(
        functools.partial(kernel, nz, ny, nx, widths, n_b),
        out_shape=jax.ShapeDtypeStruct((nz, 2, 8, columns), bf16),
        in_specs=[pl.BlockSpec(memory_space=pl.ANY)] * 3,
        out_specs=pl.BlockSpec(memory_space=pl.ANY),
        scratch_shapes=scratch,
        compiler_params=pltpu.CompilerParams(
            collective_id=0, has_side_effects=True, vmem_limit_bytes=67_043_328
        ),
        name="swiglu",
    )(tokens, gate_weight, up_weight)
    return hidden.reshape(nz * 16, columns)


def solution(mesh):
    rows, cols = mesh.shape["row"], mesh.shape["col"]
    nx, ny = 2, rows // 4
    return jax.shard_map(
        functools.partial(local, cols // 2, ny, nx),
        mesh=mesh,
        in_specs=(P("row", "col"), P("col", "row"), P("col", "row")),
        out_specs=P(None, "row"),
        check_vma=False,
    )
```

```python
import functools

import jax
import jax.numpy as jnp
from jax import lax
from jax.experimental import pallas as pl
from jax.experimental.pallas import tpu as pltpu
from jax.sharding import PartitionSpec as P

LANE = 128
B_TILES = (3, 2)
A_TILES = (4, 4)
STRIDE = 2


def kernel(nz, ny, nx, widths, n_b, tok_hbm, gate_hbm, up_hbm, hid, *scratch):
    scratch = list(scratch)
    take = scratch.pop
    tok, wg, wu = take(0), take(0), take(0)
    n_s = len(widths)
    part = [take(0) for _ in range(n_s)]
    slot = [take(0) for _ in range(n_s)]
    extra = [take(0) for _ in range(n_s)]
    total = [take(0) for _ in range(n_b)]
    load_sem, tok_send, tok_recv, pass_send, pass_recv = [take(0) for _ in range(5)]
    rs_send, rs_recv, x_send, x_recv = [take(0) for _ in range(4)]
    ag_send, ag_recv, agx_send, agx_recv = [take(0) for _ in range(4)]

    row, col = lax.axis_index("row"), lax.axis_index("col")
    core = lax.rem(row, 2)
    y = lax.rem(row // 2, ny)
    xh = row // (2 * ny)
    z = col // 2
    xl = lax.rem(col, 2)
    other = 1 - xl
    sign = (1 - 2 * core, 2 * core - 1)
    hops = (nz // 2, nz - 1 - nz // 2)

    def at_z(d, t):
        return lax.rem(z + sign[d] * t + 2 * nz, nz)

    def z_id(d, t):
        return {"col": at_z(d, t) * 2 + xl}

    def row_of(dx, dy):
        return (lax.rem(xh + dx + nx, nx) * ny + lax.rem(y + dy + ny, ny)) * 2 + core

    x_id = {"col": z * 2 + other}
    partner = {"row": row + 1 - 2 * core}

    def remote(src, dst, send, recv, device):
        return pltpu.make_async_remote_copy(
            src_ref=src, dst_ref=dst, send_sem=send, recv_sem=recv,
            device_id=device, device_id_type=pl.DeviceIdType.MESH,
        )

    loads = [
        pltpu.make_async_copy(tok_hbm, tok.at[row], load_sem.at[0]),
        pltpu.make_async_copy(gate_hbm, wg, load_sem.at[1]),
        pltpu.make_async_copy(up_hbm, wu, load_sem.at[2]),
    ]
    for copy in loads:
        copy.start()

    offsets = [(dx, dy) for dx in range(nx) for dy in range(ny) if dx or dy]
    peers = [{"row": row_of(dx, dy)} for dx, dy in offsets]
    greet = peers + [partner, x_id]
    near = sorted({(d, t) for d in (0, 1) for t in range(1, STRIDE + 1)})
    greet += [z_id(d, t) for d, t in near]
    barrier = pltpu.get_barrier_semaphore()
    for device in greet:
        pl.semaphore_signal(barrier, inc=1, device_id=device, device_id_type=pl.DeviceIdType.MESH)
    with jax.named_scope("greet"):
        pl.semaphore_wait(barrier, len(greet))

    with jax.named_scope("load"):
        loads[0].wait()
    for o, device in reversed(list(enumerate(peers))):
        remote(tok.at[row], tok.at[row], tok_send, tok_recv.at[o], device).start()
    remote(tok.at[row], tok.at[row], pass_send, pass_recv, partner).start()
    for o, (dx, dy) in enumerate(offsets):
        src = row_of(-dx, -dy)
        with jax.named_scope(f"tok{o}"):
            remote(tok.at[src], tok.at[src], tok_send, tok_recv.at[o], peers[o]).wait_recv()
        remote(tok.at[src], tok.at[src], pass_send, pass_recv, partner).start()
    all_passed = tok.at[pl.ds(0, len(peers) + 1)]
    with jax.named_scope("passed"):
        remote(all_passed, all_passed, pass_send, pass_recv, partner).wait_recv()
    with jax.named_scope("weights"):
        loads[1].wait()
        loads[2].wait()
    n_rows, rows_each, depth = tok.shape
    x = tok[...].reshape(n_rows * rows_each, depth)

    starts = [sum(widths[:i]) for i in range(n_s)]

    def multiply(i):
        w = widths[i]
        for half, ref in enumerate((wg, wu)):
            y_ = jnp.dot(x, ref[:, starts[i] : starts[i] + w], preferred_element_type=jnp.float32)
            part[i][:, :, :, half * w : (half + 1) * w] = y_.reshape(nz, 2, 8, w)

    order = [(d, t) for t in range(hops[0], 0, -1) for d in (0, 1) if t <= hops[d]] + [(0, 0)]
    place = {key: n for n, key in enumerate(order)}

    def index(d, t):
        return d * hops[0] + t - 1

    def rs(i, d, t, src):
        n = index(d, t)
        return remote(src, slot[i].at[n], rs_send.at[i], rs_recv.at[i, n], z_id(d, 1))

    def xs(i, n):
        d, t = order[n]
        return remote(part[i].at[at_z(d, t), other], extra[i].at[n], x_send.at[i], x_recv.at[i, n], x_id)

    def own(i, d, t):
        return part[i].at[at_z(d, t)] if i < n_b else part[i].at[at_z(d, t), xl]

    def step(i, d, t):
        ref = own(i, d, t)
        if i >= n_b:
            n = place[d, t]
            xs(i, n).wait_recv()
            ref[...] = ref[...] + extra[i][n]
        if t < hops[d]:
            n = index(d, t + 1)
            rs(i, d, t + 1, slot[i].at[n]).wait_recv()
            slot[i][n] = slot[i][n] + ref[...]
            ref = slot[i].at[n]
        rs(i, d, t, ref).start()

    for i in range(n_s):
        with jax.named_scope(f"mul{i}"):
            multiply(i)
        if i < n_b:
            for d in (0, 1):
                step(i, d, hops[d])
    for n in range(len(order)):
        for i in range(n_b, n_s):
            xs(i, n).start()
    for t in range(hops[0], 0, -1):
        for i in range(n_s):
            for d in (0, 1):
                if t > hops[d] or (i < n_b and t == hops[d]):
                    continue
                with jax.named_scope(f"rs{t}s{i}d{d}"):
                    step(i, d, t)

    def arrived(i):
        if hops[1]:
            ends = (0, 1)
        else:
            ends = (0,)
        for d in ends:
            rs(i, d, 1, slot[i].at[index(d, 1)]).wait_recv()
        value = slot[i][index(0, 1)]
        if hops[1]:
            value = value + slot[i][index(1, 1)]
        return value + own(i, 0, 0)[...]

    def finish(i, value):
        w = widths[i]
        gate, up = value[:, :w], value[:, w:]
        hid[z * 2 + xl, :, starts[i] : starts[i] + w] = (gate / (1.0 + jnp.exp(-gate)) * up).astype(jnp.bfloat16)

    for i in range(n_b):
      with jax.named_scope(f"tot{i}"):
        total[i][...] = arrived(i)
        remote(total[i].at[other], extra[i], x_send.at[i], x_recv.at[i, 0], x_id).start()
    for i in range(n_b, n_s):
        n = place[0, 0]
        with jax.named_scope(f"fin{i}"):
            xs(i, n).wait_recv()
            finish(i, arrived(i) + extra[i][n])
    for i in range(n_b):
        with jax.named_scope(f"fin{i}"):
            remote(total[i].at[other], extra[i], x_send.at[i], x_recv.at[i, 0], x_id).wait_recv()
            finish(i, total[i][xl] + extra[i][...])

    def along(src, d, j, k):
        ref = hid.at[src * 2 + xl]
        return remote(ref, ref, ag_send, ag_recv.at[index(d, j)], z_id(d, k))

    def across(src, side, n):
        ref = hid.at[src * 2 + side]
        return remote(ref, ref, agx_send, agx_recv.at[n], x_id)

    def spread(src, d, j):
        for k in range(STRIDE, 0, -1):
            if j + k <= hops[d]:
                along(src, d, j + k, k).start()

    last = nz - 1
    for d in (0, 1):
        spread(z, d, 0)
    across(z, xl, last).start()
    arrivals = [(j, d) for j in range(1, hops[0] + 1) for d in (0, 1) if j <= hops[d]]
    for j, d in arrivals:
        src = at_z(d, -j)
        with jax.named_scope(f"ag{j}d{d}"):
            along(src, d, j, 1).wait_recv()
        if j % STRIDE == 0:
            spread(src, d, j)
        across(src, xl, index(d, j)).start()
    with jax.named_scope("mir"):
        across(z, other, last).wait_recv()
    for j, d in arrivals:
        with jax.named_scope(f"mir{j}d{d}"):
            across(at_z(d, -j), other, index(d, j)).wait_recv()

    def sent(ref, sem):
        pltpu.make_async_copy(ref, ref, sem).wait()

    with jax.named_scope("sent"):
        sent(tok.at[pl.ds(0, len(peers))], tok_send)
        sent(all_passed, pass_send)
        for i in range(n_s):
            sent(slot[i], rs_send.at[i])
            sent(extra[i], x_send.at[i])
        sent(hid.at[pl.ds(0, nz - 1)], ag_send)
        sent(hid.at[pl.ds(0, nz)], agx_send)


def local(nz, ny, nx, tokens, gate_weight, up_weight):
    rows_each, depth = tokens.shape
    columns = gate_weight.shape[1]
    tiles = B_TILES + A_TILES
    widths = tuple(LANE * t for t in tiles)
    n_b = len(B_TILES)
    n_s = len(tiles)
    steps = nz - 1
    f32, bf16 = jnp.float32, jnp.bfloat16
    dma = pltpu.SemaphoreType.DMA
    n_peers = nx * ny - 1
    lead = [(2,) if i < n_b else () for i in range(n_s)]
    scratch = [
        pltpu.VMEM((2 * nx * ny, rows_each, depth), bf16),
        pltpu.VMEM((depth, columns), bf16),
        pltpu.VMEM((depth, columns), bf16),
    ]
    scratch += [pltpu.VMEM((nz, 2, 8, 2 * w), f32) for w in widths]
    scratch += [pltpu.VMEM((steps, *lead[i], 8, 2 * w), f32) for i, w in enumerate(widths)]
    scratch += [pltpu.VMEM((8, 2 * w) if i < n_b else (nz, 8, 2 * w), f32) for i, w in enumerate(widths)]
    scratch += [pltpu.VMEM((2, 8, 2 * w), f32) for w in widths[:n_b]]
    scratch += [dma((3,)), dma, dma((n_peers,)), dma, dma]
    scratch += [dma((n_s,)), dma((n_s, steps)), dma((n_s,)), dma((n_s, nz))]
    scratch += [dma, dma((steps,)), dma, dma((nz,))]
    hidden = pl.pallas_call(
        functools.partial(kernel, nz, ny, nx, widths, n_b),
        out_shape=pltpu.VMEM((2 * nz, 8, columns), bf16),
        in_specs=[pl.BlockSpec(memory_space=pl.ANY)] * 3,
        out_specs=pl.BlockSpec(memory_space=pltpu.VMEM),
        scratch_shapes=scratch,
        compiler_params=pltpu.CompilerParams(
            collective_id=0, has_side_effects=True, vmem_limit_bytes=66_187_264
        ),
        name="swiglu",
    )(tokens, gate_weight, up_weight)
    return hidden.reshape(nz * 16, columns)


def solution(mesh):
    rows, cols = mesh.shape["row"], mesh.shape["col"]
    nx, ny = 2, rows // 4
    return jax.shard_map(
        functools.partial(local, cols // 2, ny, nx),
        mesh=mesh,
        in_specs=(P("row", "col"), P("col", "row"), P("col", "row")),
        out_specs=P(None, "row"),
        check_vma=False,
    )
```
